32 devices in a mesh: rep: 4 (over y, x), fsdp: 8 (over z, core).
Axes of the slice: x: 2, y: 2, z: 4, core: 2. Of those that a mesh axis runs over, the one named last changes fastest.
Arguments:
- home_tokens: bfloat16 [4, 8, 1024, 1024], P('rep', None, 'fsdp'), may hold values from -6 to 6
- home_encoder: bfloat16 [4, 8, 512, 1024], P('rep', None, 'fsdp'), may hold values from -6 to 6
- out_grad: bfloat16 [4, 8, 1024, 1024], P('rep', 'fsdp'), may hold values from -6 to 6
- lengths: int32 [4, 8], P('rep'), may hold values from 1 to 1024, 6144 in all within a row
- enc_lengths: int32 [4, 8], P('rep'), may hold values from 1 to 512, 3072 in all within a row
- seq_order: int32 [4, 8], P('rep'), may hold values from 0 to 7, each once within a row
- attn_master: float32 [8, 1024, 1024], P(None, 'fsdp'), may hold values from -2 to 2
- ffin_master: float32 [2, 1024, 2816], P(None, 'fsdp'), may hold values from -0.1875 to 0.1875
- ffout_master: float32 [1024, 2816], P('fsdp'), may hold values from -0.109375 to 0.109375
- gain_master: float32 [3, 1024], P(None, 'fsdp'), may hold values from 0.5 to 1.5
- decays: float32 [4], replicated, may hold values from 0.4 to 0.6
- attn_left: float32 [8, 16, 16, 4096], P(None, 'fsdp'), may hold values from -0.15 to 2, as said below
- attn_right: float32 [8, 16, 16, 4096], P(None, 'fsdp'), may hold values from -0.15 to 2, as said below
- attn_left_root: float32 [8, 16, 16, 4096], P(None, 'fsdp'), may hold values from -0.15 to 2, as said below
- attn_right_root: float32 [8, 16, 16, 4096], P(None, 'fsdp'), may hold values from -0.15 to 2, as said below
- ffin_left: float32 [2, 16, 44, 4096], P(None, 'fsdp'), may hold values from -0.15 to 2, as said below
- ffin_right: float32 [2, 16, 44, 4096], P(None, 'fsdp'), may hold values from -0.15 to 2, as said below
- ffin_left_root: float32 [2, 16, 44, 4096], P(None, 'fsdp'), may hold values from -0.15 to 2, as said below
- ffin_right_root: float32 [2, 16, 44, 4096], P(None, 'fsdp'), may hold values from -0.15 to 2, as said below
- ffout_left: float32 [16, 44, 4096], P('fsdp'), may hold values from -0.15 to 2, as said below
- ffout_right: float32 [16, 44, 4096], P('fsdp'), may hold values from -0.15 to 2, as said below
- ffout_left_root: float32 [16, 44, 4096], P('fsdp'), may hold values from -0.15 to 2, as said below
- ffout_right_root: float32 [16, 44, 4096], P('fsdp'), may hold values from -0.15 to 2, as said below
- gain_stats: float32 [3, 1024], P(None, 'fsdp'), may hold values from 0.5 to 2
Outputs:
- out_tokens: bfloat16 [4, 8, 1024, 1024], P('rep', 'fsdp')
- token_grad: bfloat16 [4, 8, 1024, 1024], P('rep', None, 'fsdp')
- encoder_grad: bfloat16 [4, 8, 512, 1024], P('rep', None, 'fsdp')
- attn_grad: float32 [8, 1024, 1024], P(None, 'fsdp')
- ffin_grad: float32 [2, 1024, 2816], P(None, 'fsdp')
- ffout_grad: float32 [1024, 2816], P('fsdp')
- gain_grad: float32 [3, 1024], P(None, 'fsdp')
- attn_update: float32 [8, 1024, 1024], P(None, 'fsdp')
- ffin_update: float32 [2, 1024, 2816], P(None, 'fsdp')
- ffout_update: float32 [1024, 2816], P('fsdp')
- gain_update: float32 [3, 1024], P(None, 'fsdp')
- attn_left_new: float32 [8, 16, 16, 4096], P(None, 'fsdp')
- attn_right_new: float32 [8, 16, 16, 4096], P(None, 'fsdp')
- ffin_left_new: float32 [2, 16, 44, 4096], P(None, 'fsdp')
- ffin_right_new: float32 [2, 16, 44, 4096], P(None, 'fsdp')
- ffout_left_new: float32 [16, 44, 4096], P('fsdp')
- ffout_right_new: float32 [16, 44, 4096], P('fsdp')
- gain_stats_new: float32 [3, 1024], P(None, 'fsdp')
The draws below stay inside these ranges and needn't reach their ends.
Inputs may be any that keep to these rules, and one draw needn't show every extreme that they name: Row r lists the decoder lengths of the 8 sequences of group r. `enc_lengths`: row r lists the encoder lengths of the 8 sequences of group r. `seq_order`: each row is a permutation of the group's sequences. `attn_left`: each row of the last dimension is a symmetric block. `attn_right`: each row of the last dimension is a symmetric block. `attn_left_root`: each row of the last dimension is a symmetric block. `attn_right_root`: each row of the last dimension is a symmetric block. `ffin_left`: each row of the last dimension is a symmetric block. `ffin_right`: each row of the last dimension is a symmetric block. `ffin_left_root`: each row of the last dimension is a symmetric block. `ffin_right_root`: each row of the last dimension is a symmetric block. `ffout_left`: each row of the last dimension is a symmetric block. `ffout_right`: each row of the last dimension is a symmetric block. `ffout_left_root`: each row of the last dimension is a symmetric block. `ffout_right_root`: each row of the last dimension is a symmetric block.
All inputs are finite; a program needn't handle non-finite values.
Results may differ from the reference program's by a relative error of at most 0.029.
The reference program's roundings to bfloat16 on the way count: a program that leaves them out, or rounds other values in their place, can miss the bound.
Values may be sent and summed in bfloat16 or wider, within the bound.
A program may use at most 448 MiB of HBM per device.

```python
import math
import jax
import jax.numpy as jnp
import numpy as np
from jax import lax

D = 1024
HEADS = 16
HEAD = 64
FF = 2816
TILE = 64
SEQ_LEN = 1024
ENC_LEN = 512
QROWS = 512
SEQ_GRP = 8
N_REP = 4


def square_tiles(key, leading, spread):
    key_diag, key_off = jax.random.split(key)
    tile_shape = leading + (TILE, TILE)
    diagonal = jnp.exp(jax.random.uniform(key_diag, leading + (TILE,), jnp.float32, -0.6931472, 0.6931472))
    offdiag = jax.random.uniform(key_off, tile_shape, jnp.float32, -spread, spread)
    offdiag = 0.5 * (offdiag + jnp.swapaxes(offdiag, -1, -2))
    identity = jnp.eye(TILE, dtype=jnp.float32)
    tiles = offdiag * (1.0 - identity) + identity * diagonal[..., None]
    return tiles.reshape(leading + (TILE * TILE,))


def draw_attn_master(key, part):
    folded = jax.random.fold_in(key, 11)
    raw_values = jnp.clip(jax.random.normal(folded, (8, D, D), jnp.float32), -3.0, 3.0)
    fan_ins = jnp.array([D * HEAD / 4.0, D * 1.0, D * 1.0, D / 8.0, D * HEAD / 4.0, D * 1.0, D * 1.0, D / 8.0], jnp.float32)
    return raw_values * lax.rsqrt(fan_ins)[:, None, None]


def draw_attn_left(key, part):
    return square_tiles(jax.random.fold_in(key, 21), (8, D // TILE, D // TILE), 0.15)


def draw_attn_right(key, part):
    return square_tiles(jax.random.fold_in(key, 22), (8, D // TILE, D // TILE), 0.15)


def draw_attn_left_root(key, part):
    return square_tiles(jax.random.fold_in(key, 23), (8, D // TILE, D // TILE), 0.15)


def draw_attn_right_root(key, part):
    return square_tiles(jax.random.fold_in(key, 24), (8, D // TILE, D // TILE), 0.15)


def draw_ffin_left(key, part):
    return square_tiles(jax.random.fold_in(key, 31), (2, D // TILE, FF // TILE), 0.15)


def draw_ffin_right(key, part):
    return square_tiles(jax.random.fold_in(key, 32), (2, D // TILE, FF // TILE), 0.15)


def draw_ffin_left_root(key, part):
    return square_tiles(jax.random.fold_in(key, 33), (2, D // TILE, FF // TILE), 0.15)


def draw_ffin_right_root(key, part):
    return square_tiles(jax.random.fold_in(key, 34), (2, D // TILE, FF // TILE), 0.15)


def draw_ffout_left(key, part):
    return square_tiles(jax.random.fold_in(key, 41), (D // TILE, FF // TILE), 0.15)


def draw_ffout_right(key, part):
    return square_tiles(jax.random.fold_in(key, 42), (D // TILE, FF // TILE), 0.15)


def draw_ffout_left_root(key, part):
    return square_tiles(jax.random.fold_in(key, 43), (D // TILE, FF // TILE), 0.15)


def draw_ffout_right_root(key, part):
    return square_tiles(jax.random.fold_in(key, 44), (D // TILE, FF // TILE), 0.15)


def block_scale(key, shape, shards, smallest, largest):
    def one(axis_at, parts):
        heights = jax.random.uniform(jax.random.fold_in(jax.random.fold_in(key, 6), axis_at), (parts,), jnp.float32, smallest / len(shards), largest / len(shards))
        return jnp.repeat(jnp.exp(heights), shape[axis_at] // parts).reshape((-1,) + (1,) * (len(shape) - axis_at - 1))

    level = one(*shards[0])
    for cut in shards[1:]:
        level = level * one(*cut)
    return level


def profile(count, total, reach, slope):
    loads = [(1 << 20) // math.isqrt(grade ** slope) + 1 for grade in range(2, count + 1)]
    spare, holding = total - reach - (count - 1), [1] * (count - 1)
    while spare > 0:
        movable = [i for i in range(count - 1) if holding[i] < reach]
        pool, left = sum([loads[i] for i in movable]), spare
        for i in movable:
            more = min(reach - holding[i], max(1, left * loads[i] // pool), spare)
            holding[i] = holding[i] + more
            spare = spare - more
    return np.array([reach] + holding)


def uneven_parts(stream_key, number_of, total, reach, slope):
    if number_of == 2:
        one = jax.random.randint(stream_key, (), max(1, total - reach), min(reach, total - 1) + 1)
        return jnp.stack([one, total - one])
    tallies = jnp.asarray(profile(number_of, total, reach, slope), jnp.int32)
    couples = (number_of - 1) // 2
    source_of, sink = tallies[1:1 + 2 * couples:2], tallies[2:2 + 2 * couples:2]
    margin = jnp.minimum(source_of - 1, reach - sink)
    moved = jax.random.randint(jax.random.fold_in(stream_key, 1), (couples,), 0, 1 << 20) % (margin + 1)
    tallies = tallies.at[1:1 + 2 * couples:2].set(source_of - moved).at[2:2 + 2 * couples:2].set(sink + moved)
    return tallies[jax.random.permutation(jax.random.fold_in(stream_key, 2), number_of)]


def noise(rng, shape, deviation, reach, shards=(), kind=jnp.bfloat16):
    values = deviation * jax.random.normal(rng, shape, jnp.float32)
    if shards:
        values = values * block_scale(rng, shape, shards, -0.22, 0.18)
    return jnp.clip(values, -reach, reach).astype(kind)


def setup_inputs(seed: int = 0) -> dict:
    key_of = jax.random.split(jax.random.key(seed), 25)
    return {
        "home_tokens": noise(key_of[0], (N_REP, SEQ_GRP, SEQ_LEN, D), 1.0, 6.0, ((0, 4), (2, 8))),
        "home_encoder": noise(key_of[1], (N_REP, SEQ_GRP, ENC_LEN, D), 1.0, 6.0, ((0, 4), (2, 8))),
        "out_grad": noise(key_of[2], (N_REP, SEQ_GRP, SEQ_LEN, D), 1.0, 6.0, ((0, 4), (1, 8))),
        "lengths": jax.vmap(lambda own: uneven_parts(own, SEQ_GRP, SEQ_GRP * SEQ_LEN * 3 // 4, SEQ_LEN, 2))(jax.random.split(key_of[3], N_REP)).reshape((N_REP, SEQ_GRP)).astype(jnp.int32),
        "enc_lengths": jax.vmap(lambda own: uneven_parts(own, SEQ_GRP, SEQ_GRP * ENC_LEN * 3 // 4, ENC_LEN, 2))(jax.random.split(key_of[4], N_REP)).reshape((N_REP, SEQ_GRP)).astype(jnp.int32),
        "seq_order": jax.vmap(lambda own: jax.random.permutation(own, SEQ_GRP))(jax.random.split(key_of[5], N_REP)).reshape((N_REP, SEQ_GRP)).astype(jnp.int32),
        "attn_master": draw_attn_master(jax.random.fold_in(key_of[24], 71), 0),
        "ffin_master": noise(key_of[7], (2, D, FF), D ** -0.5, 0.1875, ((1, 8),), jnp.float32),
        "ffout_master": noise(key_of[8], (D, FF), FF ** -0.5, 0.109375, ((0, 8),), jnp.float32),
        "gain_master": jnp.clip(1.0 + 0.1 * jax.random.normal(key_of[9], (3, D), jnp.float32), 0.5, 1.5),
        "decays": jnp.clip(jax.random.uniform(key_of[10], (4,), jnp.float32, 0.4, 0.6), 0.4, 0.6),
        "attn_left": draw_attn_left(jax.random.fold_in(key_of[24], 71), 0),
        "attn_right": draw_attn_right(jax.random.fold_in(key_of[24], 71), 0),
        "attn_left_root": draw_attn_left_root(jax.random.fold_in(key_of[24], 71), 0),
        "attn_right_root": draw_attn_right_root(jax.random.fold_in(key_of[24], 71), 0),
        "ffin_left": draw_ffin_left(jax.random.fold_in(key_of[24], 71), 0),
        "ffin_right": draw_ffin_right(jax.random.fold_in(key_of[24], 71), 0),
        "ffin_left_root": draw_ffin_left_root(jax.random.fold_in(key_of[24], 71), 0),
        "ffin_right_root": draw_ffin_right_root(jax.random.fold_in(key_of[24], 71), 0),
        "ffout_left": draw_ffout_left(jax.random.fold_in(key_of[24], 71), 0),
        "ffout_right": draw_ffout_right(jax.random.fold_in(key_of[24], 71), 0),
        "ffout_left_root": draw_ffout_left_root(jax.random.fold_in(key_of[24], 71), 0),
        "ffout_right_root": draw_ffout_right_root(jax.random.fold_in(key_of[24], 71), 0),
        "gain_stats": jnp.clip(jnp.exp(math.log(2.0) - 1.3862944 * jax.random.uniform(key_of[23], (3, D), jnp.float32) ** block_scale(key_of[23], (3, D), ((1, 8),), -0.2, 0.2)), 0.5, 2.0),
    }


@jax.custom_vjp
def low(v):
    return lax.optimization_barrier(v.astype(jnp.bfloat16)).astype(jnp.float32)

@jax.custom_vjp
def low_back(v):
    return v

def low_keep(v):
    return (low(v), None)

def low_pass(kept, grad):
    return (grad,)

def back_keep(v):
    return (v, None)

def back_low(kept, grad):
    return (low(grad),)
low.defvjp(low_keep, low_pass)
low_back.defvjp(back_keep, back_low)
highest = lax.Precision.HIGHEST
norm_eps = 1e-06
stat_eps = 1e-06
masked_score = -1e+30

def product(left_side, right_side):
    return jnp.dot(left_side, right_side, precision=highest)

def rms_scale(inputs, gain_row):
    return inputs * lax.rsqrt(lax.optimization_barrier(jnp.mean(inputs * inputs, axis=-1, keepdims=True)) + norm_eps) * gain_row

def gelu_tanh(inputs):
    return 0.5 * inputs * (1.0 + jnp.tanh(0.7978845608 * (inputs + 0.044715 * inputs * inputs * inputs)))

def attend(queries, key_rows, value_rows, key_limit, causal):
    query_count = queries.shape[0]
    key_count = key_rows.shape[0]
    blocks = query_count // QROWS
    query_blocks = queries.reshape(blocks, QROWS, HEADS, HEAD)
    key_heads = key_rows.reshape(key_count, HEADS, HEAD)
    value_heads = value_rows.reshape(key_count, HEADS, HEAD)
    key_pos = jnp.arange(key_count, dtype=jnp.int32)

    def one_block(block_pair):
        query_block, first_row = block_pair
        scores = low_back(jnp.einsum('qhd,khd->hqk', query_block, key_heads, precision=highest))
        allowed = key_pos[None, :] < key_limit
        if causal:
            query_pos = first_row + jnp.arange(QROWS, dtype=jnp.int32)
            allowed = allowed & (key_pos[None, :] <= query_pos[:, None])
        scores = jnp.where(allowed[None], scores, masked_score)
        row_max = lax.optimization_barrier(jnp.max(scores, axis=-1, keepdims=True))
        exp_scores = jnp.exp(scores - row_max)
        soft_weights = exp_scores / lax.optimization_barrier(jnp.sum(exp_scores, axis=-1, keepdims=True))
        return jnp.einsum('hqk,khd->qhd', low(soft_weights), value_heads, precision=highest)
    starts = jnp.arange(blocks, dtype=jnp.int32) * QROWS
    blended = lax.map(jax.checkpoint(one_block), (query_blocks, starts))
    return blended.reshape(query_count, HEADS * HEAD)

def layer(tokens, encoder, attn_weights, ffin_weights, ffout_weights, gain_rows, length, enc_length):
    attn_low = low(attn_weights)
    ffin_low = low(ffin_weights)
    ffout_low = low(ffout_weights)
    gain_low = low(gain_rows)
    normed_one = low(rms_scale(tokens, gain_low[0]))
    self_query = low_back(low(product(normed_one, attn_low[0])))
    self_key = low_back(low(product(normed_one, attn_low[1])))
    self_value = low_back(low(product(normed_one, attn_low[2])))
    self_att = low_back(low(attend(self_query, self_key, self_value, length, True)))
    hidden_one = tokens + low_back(product(self_att, attn_low[3]))
    normed_two = low(rms_scale(hidden_one, gain_low[1]))
    cross_query = low_back(low(product(normed_two, attn_low[4])))
    cross_key = low_back(low(product(encoder, attn_low[5])))
    cross_value = low_back(low(product(encoder, attn_low[6])))
    cross_att = low_back(low(attend(cross_query, cross_key, cross_value, enc_length, False)))
    hidden_two = hidden_one + low_back(product(cross_att, attn_low[7]))
    normed_three = low(rms_scale(hidden_two, gain_low[2]))
    gate_part = low_back(product(normed_three, ffin_low[0]))
    up_part = low_back(product(normed_three, ffin_low[1]))
    activated = low(gelu_tanh(gate_part) * up_part)
    result = hidden_two + low_back(product(activated, ffout_low.T))
    positions = jnp.arange(SEQ_LEN, dtype=jnp.int32)
    return result * (positions < length).astype(result.dtype)[:, None]

def tile_view(matrix):
    leading = matrix.shape[:-2]
    row_count, col_count = (matrix.shape[-2], matrix.shape[-1])
    splitted = matrix.reshape(leading + (row_count // TILE, TILE, col_count // TILE, TILE))
    return jnp.swapaxes(splitted, -3, -2)

def untile(tile_grid):
    leading = tile_grid.shape[:-4]
    row_blocks, col_blocks = (tile_grid.shape[-4], tile_grid.shape[-3])
    restored = jnp.swapaxes(tile_grid, -3, -2)
    return restored.reshape(leading + (row_blocks * TILE, col_blocks * TILE))

def precondition(gradient, left_stat, right_stat, left_root, right_root, decay_rate):
    tile_grid = tile_view(gradient)
    square = tile_grid.shape
    flat_shape = square[:-2] + (TILE * TILE,)
    left_stat = left_stat.reshape(square)
    right_stat = right_stat.reshape(square)
    left_root = left_root.reshape(square)
    right_root = right_root.reshape(square)
    scaled = tile_grid * lax.rsqrt(lax.optimization_barrier(jnp.mean(tile_grid * tile_grid, axis=(-2, -1), keepdims=True)) + stat_eps)
    left_new = decay_rate * left_stat + (1.0 - decay_rate) * jnp.einsum('...ij,...kj->...ik', scaled, scaled, precision=highest) / TILE
    right_new = decay_rate * right_stat + (1.0 - decay_rate) * jnp.einsum('...ji,...jk->...ik', scaled, scaled, precision=highest) / TILE
    shaped = jnp.einsum('...ij,...jk->...ik', left_root, scaled, precision=highest)
    shaped = jnp.einsum('...ij,...jk->...ik', shaped, right_root, precision=highest)
    direction = shaped * lax.rsqrt(lax.optimization_barrier(jnp.mean(shaped * shaped, axis=(-2, -1), keepdims=True)) + stat_eps)
    return (untile(direction), left_new.reshape(flat_shape), right_new.reshape(flat_shape))

def update_gains(gradient, gain_stat, decay_rate):
    blocks = gradient.reshape(gradient.shape[0], gradient.shape[1] // TILE, TILE)
    scaled = blocks * lax.rsqrt(lax.optimization_barrier(jnp.mean(blocks * blocks, axis=-1, keepdims=True)) + stat_eps)
    stat_new = decay_rate * gain_stat.reshape(blocks.shape) + (1.0 - decay_rate) * scaled * scaled
    direction = scaled * lax.rsqrt(stat_new + stat_eps)
    return (direction.reshape(gradient.shape), stat_new.reshape(gradient.shape))

def reference(home_tokens, home_encoder, out_grad, lengths, enc_lengths, seq_order, attn_master, ffin_master, ffout_master, gain_master, decays, attn_left, attn_right, attn_left_root, attn_right_root, ffin_left, ffin_right, ffin_left_root, ffin_right_root, ffout_left, ffout_right, ffout_left_root, ffout_right_root, gain_stats):
    slot_total = N_REP * SEQ_GRP
    flat_order = seq_order.reshape(slot_total)
    flat_cot = out_grad.reshape(slot_total, SEQ_LEN, D)

    def one_slot(totals, slot_index):
        group_index = slot_index // SEQ_GRP
        sequence = flat_order[slot_index]
        tokens = home_tokens[group_index, sequence].astype(jnp.float32)
        encoder = home_encoder[group_index, sequence].astype(jnp.float32)
        length = lengths[group_index, sequence]
        enc_length = enc_lengths[group_index, sequence]

        def forward_slot(tokens, encoder, attn_weights, ffin_weights, ffout_weights, gain_rows):
            return layer(tokens, encoder, attn_weights, ffin_weights, ffout_weights, gain_rows, length, enc_length)
        output, pull_back = jax.vjp(forward_slot, tokens, encoder, attn_master, ffin_master, ffout_master, gain_master)
        gradients = pull_back(flat_cot[slot_index].astype(output.dtype))
        totals = tuple((running + fresh for running, fresh in zip(totals, gradients[2:])))
        return (totals, (output.astype(jnp.bfloat16), gradients[0].astype(jnp.bfloat16), gradients[1].astype(jnp.bfloat16)))
    initial = (jnp.zeros_like(attn_master), jnp.zeros_like(ffin_master), jnp.zeros_like(ffout_master), jnp.zeros_like(gain_master))
    totals, slot_results = lax.scan(one_slot, initial, jnp.arange(slot_total, dtype=jnp.int32))
    outputs, token_grads, encoder_grads = slot_results
    inverse = jnp.argsort(seq_order, axis=1)
    out_tokens = outputs.reshape(N_REP, SEQ_GRP, SEQ_LEN, D)
    token_grad = jnp.take_along_axis(token_grads.reshape(N_REP, SEQ_GRP, SEQ_LEN, D), inverse[:, :, None, None], axis=1)
    encoder_grad = jnp.take_along_axis(encoder_grads.reshape(N_REP, SEQ_GRP, ENC_LEN, D), inverse[:, :, None, None], axis=1)
    attn_grad, ffin_grad, ffout_grad, gain_grad = totals
    attn_update, attn_left_new, attn_right_new = precondition(attn_grad, attn_left, attn_right, attn_left_root, attn_right_root, decays[0])
    ffin_update, ffin_left_new, ffin_right_new = precondition(ffin_grad, ffin_left, ffin_right, ffin_left_root, ffin_right_root, decays[1])
    ffout_update, ffout_left_new, ffout_right_new = precondition(ffout_grad, ffout_left, ffout_right, ffout_left_root, ffout_right_root, decays[2])
    gain_update, gain_stats_new = update_gains(gain_grad, gain_stats, decays[3])
    return (out_tokens, token_grad, encoder_grad, attn_grad, ffin_grad, ffout_grad, gain_grad, attn_update, ffin_update, ffout_update, gain_update, attn_left_new, attn_right_new, ffin_left_new, ffin_right_new, ffout_left_new, ffout_right_new, gain_stats_new)
```

```python
import functools

import jax
import jax.numpy as jnp
from jax import lax
from jax.experimental import pallas as pl
from jax.experimental.pallas import tpu as pltpu
from jax.sharding import PartitionSpec as P

D = 1024
HEADS = 16
HEAD = 64
TILE = 64
SEQ_LEN = 1024
ENC_LEN = 512


norm_eps = 1e-06
stat_eps = 1e-06
masked_score = -1e30


def rms_scale(inputs, gain_row):
    return (
        inputs * lax.rsqrt(jnp.mean(inputs * inputs, axis=-1, keepdims=True) + norm_eps) * gain_row
    )


def gelu_tanh(inputs):
    return (
        0.5
        * inputs
        * (1.0 + jnp.tanh(0.7978845608 * (inputs + 0.044715 * inputs * inputs * inputs)))
    )


def gated_unit(gate_part, up_part):
    return gelu_tanh(gate_part) * up_part


def lookup(table_row, chosen):
    slot_ids = jnp.arange(table_row.shape[0], dtype=jnp.int32)
    return jnp.sum(jnp.where(chosen[:, None] == slot_ids[None, :], table_row[None, :], 0), axis=1)


def update_gains(gradient, gain_stat, decay_rate):
    blocks = gradient.reshape(gradient.shape[0], gradient.shape[1] // TILE, TILE)
    scaled = blocks * lax.rsqrt(jnp.mean(blocks * blocks, axis=-1, keepdims=True) + stat_eps)
    stat_new = decay_rate * gain_stat.reshape(blocks.shape) + (1.0 - decay_rate) * scaled * scaled
    direction = scaled * lax.rsqrt(stat_new + stat_eps)
    return (direction.reshape(gradient.shape), stat_new.reshape(gradient.shape))


PAIR = 2 * HEAD
ROWS_Q = 256
KEYS_B = 256
NT = (((1,), (1,)), ((), ()))


def matmul(left_side, right_side, dims=(((1,), (0,)), ((), ()))):
    return lax.dot_general(left_side, right_side, dims, preferred_element_type=jnp.float32)


def lane_half(values, which):
    lanes = lax.broadcasted_iota(jnp.int32, values.shape, len(values.shape) - 1)
    return jnp.where((lanes < HEAD) == (which == 0), values, jnp.zeros_like(values))


def masked(scores, key_start, query_start, limit, causal):
    key_pos = key_start + lax.broadcasted_iota(jnp.int32, scores.shape, 0)
    allowed = key_pos < limit
    if causal:
        query_pos = query_start + lax.broadcasted_iota(jnp.int32, scores.shape, 1)
        allowed = allowed & (key_pos <= query_pos)
    return jnp.where(allowed, scores, masked_score)


def forward_kernel(causal, limit_ref, q_ref, k_ref, v_ref, o_ref, total_ref, vt_ref):
    limit = limit_ref[0]
    query_count, key_count = (q_ref.shape[0], k_ref.shape[0])
    vt_ref[...] = v_ref[...].T
    for first in range(0, query_count, ROWS_Q):
        span = min(first + ROWS_Q, key_count) if causal else key_count
        queries = q_ref[first : first + ROWS_Q, :]
        halves = []
        for which in range(2):
            picked = lane_half(queries, which)
            pieces = []
            for start in range(0, span, KEYS_B):
                piece = matmul(k_ref[start : start + KEYS_B, :], picked, NT)
                diagonal = causal and start + KEYS_B > first
                pieces.append(masked(piece, start, first, limit, diagonal))
            top = pieces[0].max(axis=0, keepdims=True)
            for piece in pieces[1:]:
                top = jnp.maximum(top, piece.max(axis=0, keepdims=True))
            total = jnp.zeros_like(top)
            blended = jnp.zeros((HEAD, ROWS_Q), jnp.float32)
            for number, piece in enumerate(pieces):
                weights = jnp.exp(piece - top)
                total = total + weights.sum(axis=0, keepdims=True)
                start = number * KEYS_B
                blended = blended + matmul(
                    vt_ref[which * HEAD : (which + 1) * HEAD, start : start + KEYS_B],
                    weights.astype(jnp.bfloat16),
                )
            halves.append(blended / total)
            total_ref[which : which + 1, first : first + ROWS_Q] = top + jnp.log(total)
        o_ref[first : first + ROWS_Q, :] = jnp.concatenate(halves, 0).T.astype(o_ref.dtype)


def backward_kernel(
    causal, parts, limit_ref, q_ref, k_ref, v_ref, o_ref, g_ref, total_ref, *rest
):
    outs, (dqt_ref, kt_ref, inner_ref) = (rest[:-3], rest[-3:])
    limit = limit_ref[0]
    query_count, key_count = (q_ref.shape[0], k_ref.shape[0])
    kt_ref[...] = k_ref[...].T
    for first in range(0, query_count, ROWS_Q):
        both = g_ref[first : first + ROWS_Q, :].astype(jnp.float32) * o_ref[
            first : first + ROWS_Q, :
        ].astype(jnp.float32)
        turned = both.T
        for which in range(2):
            inner_ref[which : which + 1, first : first + ROWS_Q] = turned[
                which * HEAD : (which + 1) * HEAD, :
            ].sum(axis=0, keepdims=True)
    dqt_ref[...] = jnp.zeros_like(dqt_ref)
    for start in range(0, key_count, KEYS_B):
        key_block = k_ref[start : start + KEYS_B, :]
        value_block = v_ref[start : start + KEYS_B, :]
        key_sum = jnp.zeros((KEYS_B, PAIR), jnp.float32)
        value_sum = jnp.zeros((KEYS_B, PAIR), jnp.float32)
        for first in range(start if causal else 0, query_count, ROWS_Q):
            rows = slice(first, first + ROWS_Q)
            for which in range(2):
                picked = lane_half(q_ref[rows, :], which)
                pulled = lane_half(g_ref[rows, :], which)
                scores = masked(
                    matmul(key_block, picked, NT), start, first, limit, causal and start == first
                )
                weights = jnp.exp(scores - total_ref[which : which + 1, rows])
                value_sum = value_sum + matmul(weights.astype(jnp.bfloat16), pulled)
                slopes = matmul(value_block, pulled, NT) - inner_ref[which : which + 1, rows]
                slopes = (weights * slopes).astype(jnp.bfloat16)
                key_sum = key_sum + matmul(slopes, picked)
                feats = slice(which * HEAD, (which + 1) * HEAD)
                dqt_ref[feats, rows] += matmul(kt_ref[feats, start : start + KEYS_B], slopes)
        parts(outs, start, key_sum, value_sum)
    return dqt_ref


def attention_forward(queries, keys, limit, q_at, k_at, v_at, causal):
    rows, key_rows = (queries.shape[0], keys.shape[0])
    pairs = D // PAIR
    grid_spec = pltpu.PrefetchScalarGridSpec(
        num_scalar_prefetch=1,
        grid=(pairs,),
        in_specs=[
            pl.BlockSpec((rows, PAIR), lambda p, _: (0, q_at * pairs + p)),
            pl.BlockSpec((key_rows, PAIR), lambda p, _: (0, k_at * pairs + p)),
            pl.BlockSpec((key_rows, PAIR), lambda p, _: (0, v_at * pairs + p)),
        ],
        out_specs=[
            pl.BlockSpec((rows, PAIR), lambda p, _: (0, p)),
            pl.BlockSpec((None, 8, rows), lambda p, _: (p, 0, 0)),
        ],
        scratch_shapes=[pltpu.VMEM((PAIR, key_rows), jnp.bfloat16)],
    )
    pixels = rows * key_rows * HEADS * (0.625 if causal else 1.0)
    return pl.pallas_call(
        functools.partial(forward_kernel, causal),
        grid_spec=grid_spec,
        out_shape=(
            jax.ShapeDtypeStruct((rows, D), jnp.bfloat16),
            jax.ShapeDtypeStruct((pairs, 8, rows), jnp.float32),
        ),
        cost_estimate=pl.CostEstimate(
            flops=int(pixels * 512 * 2), bytes_accessed=rows * D * 8, transcendentals=int(pixels)
        ),
    )(limit, queries, keys, keys)


def self_back(limit_ref, q_ref, k_ref, v_ref, o_ref, g_ref, total_ref, out_ref, dk_ref, dv_ref, *scratch):
    turn = pl.program_id(1)

    @pl.when(turn == 0)
    def compute():
        def keep(outs, start, key_sum, value_sum):
            dk_ref[start : start + KEYS_B, :] = key_sum.astype(jnp.bfloat16)
            dv_ref[start : start + KEYS_B, :] = value_sum.astype(jnp.bfloat16)

        dqt_ref = backward_kernel(
            True, keep, limit_ref, q_ref, k_ref, v_ref, o_ref, g_ref, total_ref, *scratch
        )
        out_ref[...] = dqt_ref[...].T.astype(jnp.bfloat16)

    @pl.when(turn == 1)
    def give_keys():
        out_ref[...] = dk_ref[...]

    @pl.when(turn == 2)
    def give_values():
        out_ref[...] = dv_ref[...]


def cross_back(limit_ref, q_ref, k_ref, v_ref, o_ref, g_ref, total_ref, dq_ref, kv_ref, dv_ref, *scratch):
    turn = pl.program_id(1)

    @pl.when(turn == 0)
    def compute():
        def keep(outs, start, key_sum, value_sum):
            kv_ref[start : start + KEYS_B, :] = key_sum.astype(jnp.bfloat16)
            dv_ref[start : start + KEYS_B, :] = value_sum.astype(jnp.bfloat16)

        dqt_ref = backward_kernel(
            False, keep, limit_ref, q_ref, k_ref, v_ref, o_ref, g_ref, total_ref, *scratch
        )
        dq_ref[...] = dqt_ref[...].T.astype(jnp.bfloat16)

    @pl.when(turn == 1)
    def give_values():
        kv_ref[...] = dv_ref[...]


def attention_backward(queries, keys, blended, grads, totals, limit, q_at, k_at, v_at, causal):
    rows, key_rows = (queries.shape[0], keys.shape[0])
    pairs = D // PAIR
    in_specs = [
        pl.BlockSpec((rows, PAIR), lambda p, t, _: (0, q_at * pairs + p)),
        pl.BlockSpec((key_rows, PAIR), lambda p, t, _: (0, k_at * pairs + p)),
        pl.BlockSpec((key_rows, PAIR), lambda p, t, _: (0, v_at * pairs + p)),
        pl.BlockSpec((rows, PAIR), lambda p, t, _: (0, p)),
        pl.BlockSpec((rows, PAIR), lambda p, t, _: (0, p)),
        pl.BlockSpec((None, 8, rows), lambda p, t, _: (p, 0, 0)),
    ]
    turned = [
        pltpu.VMEM((PAIR, rows), jnp.float32),
        pltpu.VMEM((PAIR, key_rows), jnp.bfloat16),
        pltpu.VMEM((8, rows), jnp.float32),
    ]
    kept = pltpu.VMEM((key_rows, PAIR), jnp.bfloat16)
    if causal:
        kernel, turns, scratch = (self_back, 3, [kept, kept] + turned)
        out_specs = [pl.BlockSpec((rows, PAIR), lambda p, t, _: (0, t * pairs + p))]
        out_shape = [jax.ShapeDtypeStruct((rows, 3 * D), jnp.bfloat16)]
    else:
        kernel, turns, scratch = (cross_back, 2, [kept] + turned)
        out_specs = [
            pl.BlockSpec((rows, PAIR), lambda p, t, _: (0, p)),
            pl.BlockSpec((key_rows, PAIR), lambda p, t, _: (0, t * pairs + p)),
        ]
        out_shape = [
            jax.ShapeDtypeStruct((rows, D), jnp.bfloat16),
            jax.ShapeDtypeStruct((key_rows, 2 * D), jnp.bfloat16),
        ]
    pixels = rows * key_rows * HEADS * (0.625 if causal else 1.0)
    return pl.pallas_call(
        kernel,
        grid_spec=pltpu.PrefetchScalarGridSpec(
            num_scalar_prefetch=1,
            grid=(pairs, turns),
            in_specs=in_specs,
            out_specs=out_specs,
            scratch_shapes=scratch,
        ),
        out_shape=out_shape,
        cost_estimate=pl.CostEstimate(
            flops=int(pixels * 1280 * 2), bytes_accessed=rows * D * 16, transcendentals=int(pixels)
        ),
    )(limit, queries, keys, keys, blended, grads, totals)


CHUNK = 8
HALF = TILE // 2
SIDE = 2 * TILE


def block_scale(squares):
    column = squares.sum(axis=0, keepdims=True)
    low = lane_half(column, 0).sum(axis=1, keepdims=True)
    high = lane_half(column, 1).sum(axis=1, keepdims=True)
    lanes = lax.broadcasted_iota(jnp.int32, column.shape, 1)
    mean = jnp.where(lanes < TILE, low, high) * (1.0 / (TILE * TILE))
    return lax.rsqrt(mean + stat_eps)


def swapped(values):
    return pltpu.roll(values, TILE, 1)


def mixed(low, high):
    lanes = lax.broadcasted_iota(jnp.int32, low.shape, 1)
    return jnp.where(lanes < TILE, low, high)


def shampoo_kernel(
    decay_ref, order_ref, g_ref, ls_ref, rs_ref, lr_ref, rr_ref,
    gout_ref, up_ref, ln_ref, rn_ref, lp_ref, rp_ref, lq_ref, rq_ref, n_ref, u_ref,
):
    decay = decay_ref[0]
    fresh = (1.0 - decay) * (1.0 / TILE)
    blocks = ls_ref.shape[0]
    order = order_ref[...]
    for chunk in range(0, blocks, CHUNK):
        count = min(CHUNK, blocks - chunk)
        here = slice(chunk, chunk + count)
        for piece in range(HALF):
            lanes = slice(piece * SIDE, (piece + 1) * SIDE)
            spread = pl.ds(piece, count, stride=HALF)
            lp_ref[spread, :] = lr_ref[here, lanes]
            rp_ref[spread, :] = rr_ref[here, lanes]
        for pair in range(count // 2):
            lanes = slice((chunk + 2 * pair) * TILE, (chunk + 2 * pair + 2) * TILE)
            first = slice(2 * pair * HALF, (2 * pair + 1) * HALF)
            second = slice((2 * pair + 1) * HALF, (2 * pair + 2) * HALF)
            at = pair * TILE
            raw = g_ref[:, lanes].astype(jnp.float32)
            gout_ref[:, lanes] = raw
            scaled = raw * block_scale(raw * raw)
            n_ref[at : at + TILE, :] = scaled
            scaled = scaled.astype(jnp.bfloat16)
            evens = n_ref[pl.ds(at, HALF, stride=2), :].astype(jnp.bfloat16)
            odds = n_ref[pl.ds(at + 1, HALF, stride=2), :].astype(jnp.bfloat16)
            sorted_cols = matmul(scaled, order).astype(jnp.bfloat16)
            diagonal = jnp.concatenate([lane_half(scaled, 0), lane_half(scaled, 1)], 0)
            outer = matmul(jnp.concatenate([evens, odds], 0), diagonal, NT)
            top, bottom = (outer[:HALF], outer[HALF:])
            lq_ref[first, :] = mixed(top, swapped(bottom))
            lq_ref[second, :] = mixed(swapped(top), bottom)
            gram = matmul(sorted_cols, scaled, (((0,), (0,)), ((), ())))
            rq_ref[first, :] = mixed(gram[:HALF], swapped(gram[HALF : 2 * HALF]))
            rq_ref[second, :] = mixed(swapped(gram[2 * HALF : 3 * HALF]), gram[3 * HALF :])
            left_a, left_b = (lp_ref[first, :], lp_ref[second, :])
            left = jnp.concatenate(
                [mixed(left_a, swapped(left_b)), mixed(swapped(left_a), left_b)], 0
            ).astype(jnp.bfloat16)
            wide = jnp.concatenate([lane_half(sorted_cols, 0), lane_half(sorted_cols, 1)], 0)
            shaped = matmul(left, wide).astype(jnp.bfloat16)
            right_a, right_b = (rp_ref[first, :], rp_ref[second, :])
            right = jnp.concatenate(
                [
                    lane_half(right_a, 0),
                    lane_half(swapped(right_a), 0),
                    lane_half(swapped(right_b), 1),
                    lane_half(right_b, 1),
                ],
                0,
            ).astype(jnp.bfloat16)
            shaped = matmul(shaped, right)
            direction = shaped * block_scale(shaped * shaped)
            u_ref[pl.ds(at, HALF, stride=2), :] = direction[:HALF]
            u_ref[pl.ds(at + 1, HALF, stride=2), :] = direction[HALF:]
            up_ref[:, lanes] = u_ref[at : at + TILE, :]
        for piece in range(HALF):
            lanes = slice(piece * SIDE, (piece + 1) * SIDE)
            spread = pl.ds(piece, count, stride=HALF)
            ln_ref[here, lanes] = decay * ls_ref[here, lanes] + fresh * lq_ref[spread, :]
            rn_ref[here, lanes] = decay * rs_ref[here, lanes] + fresh * rq_ref[spread, :]


def precondition(gradient, left_stat, right_stat, left_root, right_root, decay_rate, slots):
    stat_shape = left_stat.shape
    row_blocks, blocks = (stat_shape[-3], stat_shape[-2])
    steps = slots * row_blocks
    cols = blocks * TILE
    flat = (steps, blocks, TILE * TILE)
    source = lax.broadcasted_iota(jnp.int32, (SIDE, SIDE), 1)
    within = source % TILE
    source = source - within + jnp.where(within < HALF, 2 * within, 2 * within - TILE + 1)
    order = (lax.broadcasted_iota(jnp.int32, (SIDE, SIDE), 0) == source).astype(jnp.bfloat16)
    stat_spec = pl.BlockSpec((None, blocks, TILE * TILE), lambda s, _: (s, 0, 0))
    out_spec = pl.BlockSpec((None, TILE, cols), lambda s, _: (s, 0, 0))
    held = pltpu.VMEM((CHUNK * HALF, SIDE), jnp.float32)
    grads, update, left_new, right_new = pl.pallas_call(
        shampoo_kernel,
        grid_spec=pltpu.PrefetchScalarGridSpec(
            num_scalar_prefetch=1,
            grid=(steps,),
            in_specs=[
                pl.BlockSpec((SIDE, SIDE), lambda s, _: (0, 0)),
                pl.BlockSpec((TILE, cols), lambda s, _: (s % row_blocks, s // row_blocks)),
                stat_spec, stat_spec, stat_spec, stat_spec,
            ],
            out_specs=[out_spec, out_spec, stat_spec, stat_spec],
            scratch_shapes=[held] * 6,
        ),
        out_shape=(
            jax.ShapeDtypeStruct((steps, TILE, cols), jnp.float32),
            jax.ShapeDtypeStruct((steps, TILE, cols), jnp.float32),
            jax.ShapeDtypeStruct(flat, jnp.float32),
            jax.ShapeDtypeStruct(flat, jnp.float32),
        ),
        cost_estimate=pl.CostEstimate(
            flops=steps * blocks * 2000000, bytes_accessed=steps * blocks * 4096 * 34, transcendentals=0
        ),
    )(
        decay_rate.reshape(1),
        order,
        gradient,
        left_stat.reshape(flat),
        right_stat.reshape(flat),
        left_root.reshape(flat),
        right_root.reshape(flat),
    )
    full = stat_shape[:-3] + (row_blocks * TILE, cols)
    return (
        grads.reshape(full),
        update.reshape(full),
        left_new.reshape(stat_shape),
        right_new.reshape(stat_shape),
    )


def body(
    home_tokens,
    home_encoder,
    out_grad,
    lengths,
    enc_lengths,
    seq_order,
    attn_master,
    ffin_master,
    ffout_master,
    gain_master,
    decays,
    attn_left,
    attn_right,
    attn_left_root,
    attn_right_root,
    ffin_left,
    ffin_right,
    ffin_left_root,
    ffin_right_root,
    ffout_left,
    ffout_right,
    ffout_left_root,
    ffout_right_root,
    gain_stats,
):
    rows, enc_rows = (SEQ_LEN, ENC_LEN)
    order_row = seq_order[0]
    dealt_tokens, dealt_encoder = (
        lax.all_to_all(home_tokens[0][order_row], "fsdp", split_axis=0, concat_axis=1, tiled=True),
        lax.all_to_all(home_encoder[0][order_row], "fsdp", split_axis=0, concat_axis=1, tiled=True),
    )
    my_sequence = lax.dynamic_slice_in_dim(order_row, lax.axis_index("fsdp"), 1)
    dec_limit = lookup(lengths[0], my_sequence)
    enc_limit = lookup(enc_lengths[0], my_sequence)
    tokens = dealt_tokens.reshape(rows, D).astype(jnp.float32)
    encoder = dealt_encoder.reshape(enc_rows, D)
    positions = jnp.arange(SEQ_LEN, dtype=jnp.int32)
    valid_rows = (positions < dec_limit[0]).astype(jnp.float32)[:, None]

    def low(*matrices):
        return jnp.concatenate([matrix.astype(jnp.bfloat16) for matrix in matrices], -1)

    def gather(stack):
        return lax.all_gather(stack, "fsdp", axis=0, tiled=True)

    def scatter(grad):
        return lax.psum_scatter(grad.astype(jnp.bfloat16), "fsdp", scatter_dimension=0, tiled=True)

    gain_all = gather(gain_master.astype(jnp.bfloat16).T).T.astype(jnp.float32)
    self_in = gather(low(attn_master[0], attn_master[1], attn_master[2]))
    self_out = gather(low(attn_master[3]))
    cross_all = gather(low(attn_master[4], attn_master[5], attn_master[6]))
    cross_out = gather(low(attn_master[7]))
    feed_in = gather(low(ffin_master[0], ffin_master[1]))
    feed_out = gather(low(ffout_master))
    hidden_units = feed_out.shape[1]

    normed_one = rms_scale(tokens, gain_all[0]).astype(jnp.bfloat16)
    self_qkv = matmul(normed_one, self_in).astype(jnp.bfloat16)
    self_att, self_total = attention_forward(self_qkv, self_qkv, dec_limit, 0, 1, 2, True)
    hidden_one = tokens + matmul(self_att, self_out)
    normed_two = rms_scale(hidden_one, gain_all[1]).astype(jnp.bfloat16)
    cross_query = matmul(normed_two, cross_all[:, :D]).astype(jnp.bfloat16)
    cross_kv = matmul(encoder, cross_all[:, D:]).astype(jnp.bfloat16)
    cross_att, cross_total = attention_forward(cross_query, cross_kv, enc_limit, 0, 0, 1, False)
    hidden_two = hidden_one + matmul(cross_att, cross_out)
    normed_three = rms_scale(hidden_two, gain_all[2]).astype(jnp.bfloat16)
    gate_up = matmul(normed_three, feed_in)
    gate_part, up_part = (gate_up[:, :hidden_units], gate_up[:, hidden_units:])
    activated = gated_unit(gate_part, up_part).astype(jnp.bfloat16)
    result = hidden_two + matmul(activated, feed_out, NT)
    out_tokens = (result * valid_rows).astype(jnp.bfloat16).reshape(1, 1, SEQ_LEN, D)

    cols = (((0,), (0,)), ((), ()))
    grad_result = out_grad[0, 0].astype(jnp.float32) * valid_rows
    grad_branch = grad_result.astype(jnp.bfloat16)
    grad_activated = matmul(grad_branch, feed_out)
    unused, gate_pull = jax.vjp(gated_unit, gate_part, up_part)
    grad_gate, grad_up = gate_pull(grad_activated)
    grad_gate_up = low(grad_gate, grad_up)
    grad_normed = matmul(grad_gate_up, feed_in, NT)
    feed_out_part = scatter(matmul(grad_branch, activated, cols))
    feed_in_part = scatter(matmul(normed_three, grad_gate_up, cols))
    unused, norm_pull = jax.vjp(rms_scale, hidden_two, gain_all[2])
    grad_hidden, grad_gain_three = norm_pull(grad_normed)
    grad_hidden_two = grad_result + grad_hidden

    grad_cross_z = grad_hidden_two.astype(jnp.bfloat16)
    grad_cross_att = matmul(grad_cross_z, cross_out, NT).astype(jnp.bfloat16)
    cross_out_part = scatter(matmul(cross_att, grad_cross_z, cols))
    grad_cross_query, grad_cross_kv = attention_backward(
        cross_query, cross_kv, cross_att, grad_cross_att, cross_total, enc_limit, 0, 0, 1, False
    )
    grad_normed_two = matmul(grad_cross_query, cross_all[:, :D], NT)
    grad_encoder = matmul(grad_cross_kv, cross_all[:, D:], NT)
    cross_query_part = scatter(matmul(normed_two, grad_cross_query, cols))
    cross_kv_part = scatter(matmul(encoder, grad_cross_kv, cols))
    unused, norm_pull = jax.vjp(rms_scale, hidden_one, gain_all[1])
    grad_hidden, grad_gain_two = norm_pull(grad_normed_two)
    grad_hidden_one = grad_hidden_two + grad_hidden

    grad_self_z = grad_hidden_one.astype(jnp.bfloat16)
    grad_self_att = matmul(grad_self_z, self_out, NT).astype(jnp.bfloat16)
    self_out_part = scatter(matmul(self_att, grad_self_z, cols))
    (grad_self_qkv,) = attention_backward(
        self_qkv, self_qkv, self_att, grad_self_att, self_total, dec_limit, 0, 1, 2, True
    )
    self_in_part = scatter(matmul(normed_one, grad_self_qkv, cols))
    grad_normed_one = matmul(grad_self_qkv, self_in, NT)
    unused, norm_pull = jax.vjp(rms_scale, tokens, gain_all[0])
    grad_hidden, grad_gain_one = norm_pull(grad_normed_one)
    grad_tokens = grad_hidden_one + grad_hidden
    gain_part = scatter(jnp.stack([grad_gain_one, grad_gain_two, grad_gain_three], 1)).T

    back_tokens, back_encoder = (
        lax.all_to_all(
            grad_tokens.astype(jnp.bfloat16).reshape(1, SEQ_LEN, D),
            "fsdp",
            split_axis=1,
            concat_axis=0,
            tiled=True,
        ),
        lax.all_to_all(
            grad_encoder.astype(jnp.bfloat16).reshape(1, ENC_LEN, D),
            "fsdp",
            split_axis=1,
            concat_axis=0,
            tiled=True,
        ),
    )
    slot_ids = jnp.arange(order_row.shape[0], dtype=jnp.int32)
    inverse = jnp.sum(
        jnp.where(order_row[None, :] == slot_ids[:, None], slot_ids[None, :], 0), axis=1
    )
    token_grad = back_tokens[inverse][None]
    encoder_grad = back_encoder[inverse][None]

    def total(part):
        return lax.psum(part, "rep")

    attn_sum = total(
        jnp.concatenate(
            [self_in_part, self_out_part, cross_query_part, cross_kv_part, cross_out_part], 1
        )
    )
    feed_in_sum = total(feed_in_part)
    feed_out_sum = total(feed_out_part)
    gain_grad = total(gain_part).astype(jnp.float32)
    attn_grad, attn_update, attn_left_new, attn_right_new = precondition(
        attn_sum, attn_left, attn_right, attn_left_root, attn_right_root, decays[0], 8
    )
    ffin_grad, ffin_update, ffin_left_new, ffin_right_new = precondition(
        feed_in_sum, ffin_left, ffin_right, ffin_left_root, ffin_right_root, decays[1], 2
    )
    ffout_grad, ffout_update, ffout_left_new, ffout_right_new = precondition(
        feed_out_sum, ffout_left, ffout_right, ffout_left_root, ffout_right_root, decays[2], 1
    )
    gain_update, gain_stats_new = update_gains(gain_grad, gain_stats, decays[3])
    return (
        out_tokens,
        token_grad,
        encoder_grad,
        attn_grad,
        ffin_grad,
        ffout_grad,
        gain_grad,
        attn_update,
        ffin_update,
        ffout_update,
        gain_update,
        attn_left_new,
        attn_right_new,
        ffin_left_new,
        ffin_right_new,
        ffout_left_new,
        ffout_right_new,
        gain_stats_new,
    )


def solution(mesh):
    in_specs = (
        P("rep", None, "fsdp", None),
        P("rep", None, "fsdp", None),
        P("rep", "fsdp", None, None),
        P("rep", None),
        P("rep", None),
        P("rep", None),
        P(None, "fsdp", None),
        P(None, "fsdp", None),
        P("fsdp", None),
        P(None, "fsdp"),
        P(),
        P(None, "fsdp", None, None),
        P(None, "fsdp", None, None),
        P(None, "fsdp", None, None),
        P(None, "fsdp", None, None),
        P(None, "fsdp", None, None),
        P(None, "fsdp", None, None),
        P(None, "fsdp", None, None),
        P(None, "fsdp", None, None),
        P("fsdp", None, None),
        P("fsdp", None, None),
        P("fsdp", None, None),
        P("fsdp", None, None),
        P(None, "fsdp"),
    )
    out_specs = (
        P("rep", "fsdp", None, None),
        P("rep", None, "fsdp", None),
        P("rep", None, "fsdp", None),
        P(None, "fsdp", None),
        P(None, "fsdp", None),
        P("fsdp", None),
        P(None, "fsdp"),
        P(None, "fsdp", None),
        P(None, "fsdp", None),
        P("fsdp", None),
        P(None, "fsdp"),
        P(None, "fsdp", None, None),
        P(None, "fsdp", None, None),
        P(None, "fsdp", None, None),
        P(None, "fsdp", None, None),
        P("fsdp", None, None),
        P("fsdp", None, None),
        P(None, "fsdp"),
    )
    return jax.shard_map(body, mesh=mesh, in_specs=in_specs, out_specs=out_specs, check_vma=False)
```

```python
import functools

import jax
import jax.numpy as jnp
from jax import lax
from jax.experimental import pallas as pl
from jax.experimental.pallas import tpu as pltpu
from jax.sharding import PartitionSpec as P

D = 1024
HEADS = 16
HEAD = 64
TILE = 64
SEQ_LEN = 1024
ENC_LEN = 512


norm_eps = 1e-06
stat_eps = 1e-06
masked_score = -1e30


def rms_scale(inputs, gain_row):
    return (
        inputs * lax.rsqrt(jnp.mean(inputs * inputs, axis=-1, keepdims=True) + norm_eps) * gain_row
    )


def gelu_tanh(inputs):
    return (
        0.5
        * inputs
        * (1.0 + jnp.tanh(0.7978845608 * (inputs + 0.044715 * inputs * inputs * inputs)))
    )


def gated_unit(gate_part, up_part):
    return gelu_tanh(gate_part) * up_part


def swap(values, axis, size, shift):
    return lax.ppermute(values, axis, [(at, at ^ shift) for at in range(size)])


def put(buffer, piece, at, axis):
    return lax.dynamic_update_slice_in_dim(buffer, piece, at, axis)


def take(values, at, axis):
    return lax.dynamic_index_in_dim(values, at, axis, keepdims=True)


class Links:
    def __init__(self, mesh):
        self.reps, self.shards = (mesh.shape["rep"], mesh.shape["fsdp"])
        self.chips = self.shards // 2
        self.rep, self.shard = (lax.axis_index("rep"), lax.axis_index("fsdp"))
        self.chip, self.core = (self.shard // 2, self.shard % 2)

    def gather_chips(self, shard):
        rows, cols = shard.shape
        part = take(shard.reshape(self.reps, rows // self.reps, cols), self.rep, 0)
        held = jnp.zeros((self.chips,) + part.shape[1:], part.dtype)
        held = put(held, part, self.chip, 0)
        for shift in range(1, self.chips):
            held = put(held, swap(part, "fsdp", self.shards, 2 * shift), self.chip ^ shift, 0)
        return held

    def gather_rest(self, held):
        held = held[:, None]
        spread = jnp.zeros((self.chips, self.reps) + held.shape[2:], held.dtype)
        spread = put(spread, held, self.rep, 1)
        for shift in range(1, self.reps):
            spread = put(spread, swap(held, "rep", self.reps, shift), self.rep ^ shift, 1)
        spread = spread[:, None]
        full = jnp.zeros((self.chips, 2) + spread.shape[2:], held.dtype)
        full = put(full, spread, self.core, 1)
        full = put(full, swap(spread, "fsdp", self.shards, 1), 1 - self.core, 1)
        return full.reshape(-1, held.shape[-1])

    def summed(self, pieces):
        total = pieces[0].astype(jnp.float32)
        for piece in pieces[1:]:
            total = total + piece.astype(jnp.float32)
        return total.astype(jnp.bfloat16)

    def share(self, values, axis, size, stride, mine, at):
        count = values.shape[at]
        pieces = [take(values, mine, at)]
        for shift in range(1, count):
            pieces.append(swap(take(values, mine ^ shift, at), axis, size, shift * stride))
        return self.summed(pieces)

    def spread_rep(self, part):
        full = jnp.zeros((self.reps,) + part.shape, part.dtype)
        full = put(full, part[None], self.rep, 0)
        for shift in range(1, self.reps):
            full = put(full, swap(part, "rep", self.reps, shift)[None], self.rep ^ shift, 0)
        return full

    def reduce(self, grad):
        rows, cols = grad.shape
        per = rows // (self.shards * self.reps)
        grad = grad.reshape(self.chips, 2, self.reps, per, cols)
        grad = self.share(grad, "fsdp", self.shards, 1, self.core, 1)
        grad = self.share(grad, "rep", self.reps, 1, self.rep, 2)
        grad = self.share(grad, "fsdp", self.shards, 2, self.chip, 0)
        return self.spread_rep(grad.reshape(per, cols)).reshape(rows // self.shards, cols)

    def reduce_rep(self, part):
        rows, cols = part.shape
        part = self.share(part.reshape(self.reps, rows // self.reps, cols), "rep", self.reps, 1, self.rep, 0)
        return self.spread_rep(part[0]).reshape(rows, cols)

    def deal(self, home, order_row):
        held = jnp.zeros((self.shards,) + home.shape[1:], home.dtype)
        for shift in range(self.shards):
            piece = take(home, order_row[self.shard ^ shift], 0)
            if shift:
                piece = swap(piece, "fsdp", self.shards, shift)
            held = put(held, piece, self.shard ^ shift, 0)
        return held.reshape(-1, home.shape[-1])

    def back(self, grads, order_row):
        pieces = grads.reshape(self.shards, -1, grads.shape[-1])
        home = jnp.zeros(pieces.shape, pieces.dtype)
        for shift in range(self.shards):
            piece = take(pieces, self.shard ^ shift, 0)
            if shift:
                piece = swap(piece, "fsdp", self.shards, shift)
            home = put(home, piece, order_row[self.shard ^ shift], 0)
        return home[None]

    def gather_small(self, values):
        held = jnp.zeros((self.shards,) + values.shape, values.dtype)
        held = put(held, values[None], self.shard, 0)
        for shift in range(1, self.shards):
            held = put(held, swap(values, "fsdp", self.shards, shift)[None], self.shard ^ shift, 0)
        return held


def lookup(table_row, chosen):
    slot_ids = jnp.arange(table_row.shape[0], dtype=jnp.int32)
    return jnp.sum(jnp.where(chosen[:, None] == slot_ids[None, :], table_row[None, :], 0), axis=1)


def update_gains(gradient, gain_stat, decay_rate):
    blocks = gradient.reshape(gradient.shape[0], gradient.shape[1] // TILE, TILE)
    scaled = blocks * lax.rsqrt(jnp.mean(blocks * blocks, axis=-1, keepdims=True) + stat_eps)
    stat_new = decay_rate * gain_stat.reshape(blocks.shape) + (1.0 - decay_rate) * scaled * scaled
    direction = scaled * lax.rsqrt(stat_new + stat_eps)
    return (direction.reshape(gradient.shape), stat_new.reshape(gradient.shape))


PAIR = 2 * HEAD
ROWS_Q = 256
KEYS_B = 256
NT = (((1,), (1,)), ((), ()))


def matmul(left_side, right_side, dims=(((1,), (0,)), ((), ()))):
    return lax.dot_general(left_side, right_side, dims, preferred_element_type=jnp.float32)


def lane_half(values, which):
    lanes = lax.broadcasted_iota(jnp.int32, values.shape, len(values.shape) - 1)
    return jnp.where((lanes < HEAD) == (which == 0), values, jnp.zeros_like(values))


def masked(scores, key_start, query_start, limit, causal):
    key_pos = key_start + lax.broadcasted_iota(jnp.int32, scores.shape, 0)
    allowed = key_pos < limit
    if causal:
        query_pos = query_start + lax.broadcasted_iota(jnp.int32, scores.shape, 1)
        allowed = allowed & (key_pos <= query_pos)
    return jnp.where(allowed, scores, masked_score)


def forward_kernel(causal, limit_ref, q_ref, k_ref, v_ref, o_ref, total_ref, vt_ref):
    limit = limit_ref[0]
    query_count, key_count = (q_ref.shape[0], k_ref.shape[0])
    vt_ref[...] = v_ref[...].T
    for first in range(0, query_count, ROWS_Q):
        span = min(first + ROWS_Q, key_count) if causal else key_count
        queries = q_ref[first : first + ROWS_Q, :]
        halves = []
        for which in range(2):
            picked = lane_half(queries, which)
            pieces = []
            for start in range(0, span, KEYS_B):
                piece = matmul(k_ref[start : start + KEYS_B, :], picked, NT)
                diagonal = causal and start + KEYS_B > first
                pieces.append(masked(piece, start, first, limit, diagonal))
            top = pieces[0].max(axis=0, keepdims=True)
            for piece in pieces[1:]:
                top = jnp.maximum(top, piece.max(axis=0, keepdims=True))
            total = jnp.zeros_like(top)
            blended = jnp.zeros((HEAD, ROWS_Q), jnp.float32)
            for number, piece in enumerate(pieces):
                weights = jnp.exp(piece - top)
                total = total + weights.sum(axis=0, keepdims=True)
                start = number * KEYS_B
                blended = blended + matmul(
                    vt_ref[which * HEAD : (which + 1) * HEAD, start : start + KEYS_B],
                    weights.astype(jnp.bfloat16),
                )
            halves.append(blended / total)
            total_ref[which : which + 1, first : first + ROWS_Q] = top + jnp.log(total)
        o_ref[first : first + ROWS_Q, :] = jnp.concatenate(halves, 0).T.astype(o_ref.dtype)


def backward_kernel(
    causal, parts, limit_ref, q_ref, k_ref, v_ref, o_ref, g_ref, total_ref, *rest
):
    outs, (dqt_ref, kt_ref, inner_ref) = (rest[:-3], rest[-3:])
    limit = limit_ref[0]
    query_count, key_count = (q_ref.shape[0], k_ref.shape[0])
    kt_ref[...] = k_ref[...].T
    for first in range(0, query_count, ROWS_Q):
        both = g_ref[first : first + ROWS_Q, :].astype(jnp.float32) * o_ref[
            first : first + ROWS_Q, :
        ].astype(jnp.float32)
        turned = both.T
        for which in range(2):
            inner_ref[which : which + 1, first : first + ROWS_Q] = turned[
                which * HEAD : (which + 1) * HEAD, :
            ].sum(axis=0, keepdims=True)
    dqt_ref[...] = jnp.zeros_like(dqt_ref)
    for start in range(0, key_count, KEYS_B):
        key_block = k_ref[start : start + KEYS_B, :]
        value_block = v_ref[start : start + KEYS_B, :]
        key_sum = jnp.zeros((KEYS_B, PAIR), jnp.float32)
        value_sum = jnp.zeros((KEYS_B, PAIR), jnp.float32)
        for first in range(start if causal else 0, query_count, ROWS_Q):
            rows = slice(first, first + ROWS_Q)
            for which in range(2):
                picked = lane_half(q_ref[rows, :], which)
                pulled = lane_half(g_ref[rows, :], which)
                scores = masked(
                    matmul(key_block, picked, NT), start, first, limit, causal and start == first
                )
                weights = jnp.exp(scores - total_ref[which : which + 1, rows])
                value_sum = value_sum + matmul(weights.astype(jnp.bfloat16), pulled)
                slopes = matmul(value_block, pulled, NT) - inner_ref[which : which + 1, rows]
                slopes = (weights * slopes).astype(jnp.bfloat16)
                key_sum = key_sum + matmul(slopes, picked)
                feats = slice(which * HEAD, (which + 1) * HEAD)
                dqt_ref[feats, rows] += matmul(kt_ref[feats, start : start + KEYS_B], slopes)
        parts(outs, start, key_sum, value_sum)
    return dqt_ref


def attention_forward(queries, keys, limit, q_at, k_at, v_at, causal):
    rows, key_rows = (queries.shape[0], keys.shape[0])
    pairs = D // PAIR
    grid_spec = pltpu.PrefetchScalarGridSpec(
        num_scalar_prefetch=1,
        grid=(pairs,),
        in_specs=[
            pl.BlockSpec((rows, PAIR), lambda p, _: (0, q_at * pairs + p)),
            pl.BlockSpec((key_rows, PAIR), lambda p, _: (0, k_at * pairs + p)),
            pl.BlockSpec((key_rows, PAIR), lambda p, _: (0, v_at * pairs + p)),
        ],
        out_specs=[
            pl.BlockSpec((rows, PAIR), lambda p, _: (0, p)),
            pl.BlockSpec((None, 8, rows), lambda p, _: (p, 0, 0)),
        ],
        scratch_shapes=[pltpu.VMEM((PAIR, key_rows), jnp.bfloat16)],
    )
    pixels = rows * key_rows * HEADS * (0.625 if causal else 1.0)
    return pl.pallas_call(
        functools.partial(forward_kernel, causal),
        grid_spec=grid_spec,
        out_shape=(
            jax.ShapeDtypeStruct((rows, D), jnp.bfloat16),
            jax.ShapeDtypeStruct((pairs, 8, rows), jnp.float32),
        ),
        cost_estimate=pl.CostEstimate(
            flops=int(pixels * 512 * 2), bytes_accessed=rows * D * 8, transcendentals=int(pixels)
        ),
    )(limit, queries, keys, keys)


def self_back(limit_ref, q_ref, k_ref, v_ref, o_ref, g_ref, total_ref, out_ref, dk_ref, dv_ref, *scratch):
    turn = pl.program_id(1)

    @pl.when(turn == 0)
    def compute():
        def keep(outs, start, key_sum, value_sum):
            dk_ref[start : start + KEYS_B, :] = key_sum.astype(jnp.bfloat16)
            dv_ref[start : start + KEYS_B, :] = value_sum.astype(jnp.bfloat16)

        dqt_ref = backward_kernel(
            True, keep, limit_ref, q_ref, k_ref, v_ref, o_ref, g_ref, total_ref, *scratch
        )
        out_ref[...] = dqt_ref[...].T.astype(jnp.bfloat16)

    @pl.when(turn == 1)
    def give_keys():
        out_ref[...] = dk_ref[...]

    @pl.when(turn == 2)
    def give_values():
        out_ref[...] = dv_ref[...]


def cross_back(limit_ref, q_ref, k_ref, v_ref, o_ref, g_ref, total_ref, dq_ref, kv_ref, dv_ref, *scratch):
    turn = pl.program_id(1)

    @pl.when(turn == 0)
    def compute():
        def keep(outs, start, key_sum, value_sum):
            kv_ref[start : start + KEYS_B, :] = key_sum.astype(jnp.bfloat16)
            dv_ref[start : start + KEYS_B, :] = value_sum.astype(jnp.bfloat16)

        dqt_ref = backward_kernel(
            False, keep, limit_ref, q_ref, k_ref, v_ref, o_ref, g_ref, total_ref, *scratch
        )
        dq_ref[...] = dqt_ref[...].T.astype(jnp.bfloat16)

    @pl.when(turn == 1)
    def give_values():
        kv_ref[...] = dv_ref[...]


def attention_backward(queries, keys, blended, grads, totals, limit, q_at, k_at, v_at, causal):
    rows, key_rows = (queries.shape[0], keys.shape[0])
    pairs = D // PAIR
    in_specs = [
        pl.BlockSpec((rows, PAIR), lambda p, t, _: (0, q_at * pairs + p)),
        pl.BlockSpec((key_rows, PAIR), lambda p, t, _: (0, k_at * pairs + p)),
        pl.BlockSpec((key_rows, PAIR), lambda p, t, _: (0, v_at * pairs + p)),
        pl.BlockSpec((rows, PAIR), lambda p, t, _: (0, p)),
        pl.BlockSpec((rows, PAIR), lambda p, t, _: (0, p)),
        pl.BlockSpec((None, 8, rows), lambda p, t, _: (p, 0, 0)),
    ]
    turned = [
        pltpu.VMEM((PAIR, rows), jnp.float32),
        pltpu.VMEM((PAIR, key_rows), jnp.bfloat16),
        pltpu.VMEM((8, rows), jnp.float32),
    ]
    kept = pltpu.VMEM((key_rows, PAIR), jnp.bfloat16)
    if causal:
        kernel, turns, scratch = (self_back, 3, [kept, kept] + turned)
        out_specs = [pl.BlockSpec((rows, PAIR), lambda p, t, _: (0, t * pairs + p))]
        out_shape = [jax.ShapeDtypeStruct((rows, 3 * D), jnp.bfloat16)]
    else:
        kernel, turns, scratch = (cross_back, 2, [kept] + turned)
        out_specs = [
            pl.BlockSpec((rows, PAIR), lambda p, t, _: (0, p)),
            pl.BlockSpec((key_rows, PAIR), lambda p, t, _: (0, t * pairs + p)),
        ]
        out_shape = [
            jax.ShapeDtypeStruct((rows, D), jnp.bfloat16),
            jax.ShapeDtypeStruct((key_rows, 2 * D), jnp.bfloat16),
        ]
    pixels = rows * key_rows * HEADS * (0.625 if causal else 1.0)
    return pl.pallas_call(
        kernel,
        grid_spec=pltpu.PrefetchScalarGridSpec(
            num_scalar_prefetch=1,
            grid=(pairs, turns),
            in_specs=in_specs,
            out_specs=out_specs,
            scratch_shapes=scratch,
        ),
        out_shape=out_shape,
        cost_estimate=pl.CostEstimate(
            flops=int(pixels * 1280 * 2), bytes_accessed=rows * D * 16, transcendentals=int(pixels)
        ),
    )(limit, queries, keys, keys, blended, grads, totals)


CHUNK = 8
HALF = TILE // 2
SIDE = 2 * TILE


def block_scale(squares):
    column = squares.sum(axis=0, keepdims=True)
    low = lane_half(column, 0).sum(axis=1, keepdims=True)
    high = lane_half(column, 1).sum(axis=1, keepdims=True)
    lanes = lax.broadcasted_iota(jnp.int32, column.shape, 1)
    mean = jnp.where(lanes < TILE, low, high) * (1.0 / (TILE * TILE))
    return lax.rsqrt(mean + stat_eps)


def swapped(values):
    return pltpu.roll(values, TILE, 1)


def mixed(low, high):
    lanes = lax.broadcasted_iota(jnp.int32, low.shape, 1)
    return jnp.where(lanes < TILE, low, high)


def shampoo_kernel(
    decay_ref, order_ref, g_ref, ls_ref, rs_ref, lr_ref, rr_ref,
    gout_ref, up_ref, ln_ref, rn_ref, lp_ref, rp_ref, lq_ref, rq_ref, n_ref, u_ref,
):
    decay = decay_ref[0]
    fresh = (1.0 - decay) * (1.0 / TILE)
    blocks = ls_ref.shape[0]
    order = order_ref[...]
    for chunk in range(0, blocks, CHUNK):
        count = min(CHUNK, blocks - chunk)
        here = slice(chunk, chunk + count)
        for piece in range(HALF):
            lanes = slice(piece * SIDE, (piece + 1) * SIDE)
            spread = pl.ds(piece, count, stride=HALF)
            lp_ref[spread, :] = lr_ref[here, lanes]
            rp_ref[spread, :] = rr_ref[here, lanes]
        for pair in range(count // 2):
            lanes = slice((chunk + 2 * pair) * TILE, (chunk + 2 * pair + 2) * TILE)
            first = slice(2 * pair * HALF, (2 * pair + 1) * HALF)
            second = slice((2 * pair + 1) * HALF, (2 * pair + 2) * HALF)
            at = pair * TILE
            raw = g_ref[:, lanes].astype(jnp.float32)
            gout_ref[:, lanes] = raw
            scaled = raw * block_scale(raw * raw)
            n_ref[at : at + TILE, :] = scaled
            scaled = scaled.astype(jnp.bfloat16)
            evens = n_ref[pl.ds(at, HALF, stride=2), :].astype(jnp.bfloat16)
            odds = n_ref[pl.ds(at + 1, HALF, stride=2), :].astype(jnp.bfloat16)
            sorted_cols = matmul(scaled, order).astype(jnp.bfloat16)
            diagonal = jnp.concatenate([lane_half(scaled, 0), lane_half(scaled, 1)], 0)
            outer = matmul(jnp.concatenate([evens, odds], 0), diagonal, NT)
            top, bottom = (outer[:HALF], outer[HALF:])
            lq_ref[first, :] = mixed(top, swapped(bottom))
            lq_ref[second, :] = mixed(swapped(top), bottom)
            gram = matmul(sorted_cols, scaled, (((0,), (0,)), ((), ())))
            rq_ref[first, :] = mixed(gram[:HALF], swapped(gram[HALF : 2 * HALF]))
            rq_ref[second, :] = mixed(swapped(gram[2 * HALF : 3 * HALF]), gram[3 * HALF :])
            left_a, left_b = (lp_ref[first, :], lp_ref[second, :])
            left = jnp.concatenate(
                [mixed(left_a, swapped(left_b)), mixed(swapped(left_a), left_b)], 0
            ).astype(jnp.bfloat16)
            wide = jnp.concatenate([lane_half(sorted_cols, 0), lane_half(sorted_cols, 1)], 0)
            shaped = matmul(left, wide).astype(jnp.bfloat16)
            right_a, right_b = (rp_ref[first, :], rp_ref[second, :])
            right = jnp.concatenate(
                [
                    lane_half(right_a, 0),
                    lane_half(swapped(right_a), 0),
                    lane_half(swapped(right_b), 1),
                    lane_half(right_b, 1),
                ],
                0,
            ).astype(jnp.bfloat16)
            shaped = matmul(shaped, right)
            direction = shaped * block_scale(shaped * shaped)
            u_ref[pl.ds(at, HALF, stride=2), :] = direction[:HALF]
            u_ref[pl.ds(at + 1, HALF, stride=2), :] = direction[HALF:]
            up_ref[:, lanes] = u_ref[at : at + TILE, :]
        for piece in range(HALF):
            lanes = slice(piece * SIDE, (piece + 1) * SIDE)
            spread = pl.ds(piece, count, stride=HALF)
            ln_ref[here, lanes] = decay * ls_ref[here, lanes] + fresh * lq_ref[spread, :]
            rn_ref[here, lanes] = decay * rs_ref[here, lanes] + fresh * rq_ref[spread, :]


def precondition(gradient, left_stat, right_stat, left_root, right_root, decay_rate, slots):
    stat_shape = left_stat.shape
    row_blocks, blocks = (stat_shape[-3], stat_shape[-2])
    steps = slots * row_blocks
    cols = blocks * TILE
    flat = (steps, blocks, TILE * TILE)
    source = lax.broadcasted_iota(jnp.int32, (SIDE, SIDE), 1)
    within = source % TILE
    source = source - within + jnp.where(within < HALF, 2 * within, 2 * within - TILE + 1)
    order = (lax.broadcasted_iota(jnp.int32, (SIDE, SIDE), 0) == source).astype(jnp.bfloat16)
    stat_spec = pl.BlockSpec((None, blocks, TILE * TILE), lambda s, _: (s, 0, 0))
    out_spec = pl.BlockSpec((None, TILE, cols), lambda s, _: (s, 0, 0))
    held = pltpu.VMEM((CHUNK * HALF, SIDE), jnp.float32)
    grads, update, left_new, right_new = pl.pallas_call(
        shampoo_kernel,
        grid_spec=pltpu.PrefetchScalarGridSpec(
            num_scalar_prefetch=1,
            grid=(steps,),
            in_specs=[
                pl.BlockSpec((SIDE, SIDE), lambda s, _: (0, 0)),
                pl.BlockSpec((TILE, cols), lambda s, _: (s % row_blocks, s // row_blocks)),
                stat_spec, stat_spec, stat_spec, stat_spec,
            ],
            out_specs=[out_spec, out_spec, stat_spec, stat_spec],
            scratch_shapes=[held] * 6,
        ),
        out_shape=(
            jax.ShapeDtypeStruct((steps, TILE, cols), jnp.float32),
            jax.ShapeDtypeStruct((steps, TILE, cols), jnp.float32),
            jax.ShapeDtypeStruct(flat, jnp.float32),
            jax.ShapeDtypeStruct(flat, jnp.float32),
        ),
        cost_estimate=pl.CostEstimate(
            flops=steps * blocks * 2000000, bytes_accessed=steps * blocks * 4096 * 34, transcendentals=0
        ),
    )(
        decay_rate.reshape(1),
        order,
        gradient,
        left_stat.reshape(flat),
        right_stat.reshape(flat),
        left_root.reshape(flat),
        right_root.reshape(flat),
    )
    full = stat_shape[:-3] + (row_blocks * TILE, cols)
    return (
        grads.reshape(full),
        update.reshape(full),
        left_new.reshape(stat_shape),
        right_new.reshape(stat_shape),
    )


def body(
    mesh,
    home_tokens,
    home_encoder,
    out_grad,
    lengths,
    enc_lengths,
    seq_order,
    attn_master,
    ffin_master,
    ffout_master,
    gain_master,
    decays,
    attn_left,
    attn_right,
    attn_left_root,
    attn_right_root,
    ffin_left,
    ffin_right,
    ffin_left_root,
    ffin_right_root,
    ffout_left,
    ffout_right,
    ffout_left_root,
    ffout_right_root,
    gain_stats,
):
    rows, enc_rows = (SEQ_LEN, ENC_LEN)
    order_row = seq_order[0]
    links = Links(mesh)
    tie = lax.optimization_barrier
    tokens = links.deal(home_tokens[0], order_row)
    my_sequence = lax.dynamic_slice_in_dim(order_row, lax.axis_index("fsdp"), 1)
    dec_limit = lookup(lengths[0], my_sequence)
    enc_limit = lookup(enc_lengths[0], my_sequence)
    positions = jnp.arange(SEQ_LEN, dtype=jnp.int32)
    valid_rows = (positions < dec_limit[0]).astype(jnp.float32)[:, None]

    def low(*matrices):
        return jnp.concatenate([matrix.astype(jnp.bfloat16) for matrix in matrices], -1)

    def gather(stack):
        return lax.all_gather(stack, "fsdp", axis=0, tiled=True)

    def scatter(grad):
        return lax.psum_scatter(grad.astype(jnp.bfloat16), "fsdp", scatter_dimension=0, tiled=True)

    gain_all = links.gather_small(gain_master.astype(jnp.bfloat16))
    gain_all = jnp.swapaxes(gain_all, 0, 1).reshape(3, D).astype(jnp.float32)
    first = links.gather_chips(low(attn_master[0], attn_master[1], attn_master[2]))
    first, tokens, home_encoder, ffin_master, ffout_master, attn_rest = tie(
        (first, tokens, home_encoder, ffin_master, ffout_master, attn_master[3:])
    )
    tokens = tokens.astype(jnp.float32)
    self_in = links.gather_rest(first)
    encoder = links.deal(home_encoder[0], order_row)
    feed_in = gather(low(ffin_master[0], ffin_master[1]))
    feed_out = gather(low(ffout_master))
    self_out = links.gather_rest(links.gather_chips(low(attn_rest[0])))
    cross_in = links.gather_rest(links.gather_chips(low(attn_rest[1])))
    cross_kv_in = links.gather_rest(links.gather_chips(low(attn_rest[2], attn_rest[3])))
    cross_out = links.gather_rest(links.gather_chips(low(attn_rest[4])))
    hidden_units = feed_out.shape[1]

    normed_one = rms_scale(tokens, gain_all[0]).astype(jnp.bfloat16)
    self_qkv = matmul(normed_one, self_in).astype(jnp.bfloat16)
    self_att, self_total = attention_forward(self_qkv, self_qkv, dec_limit, 0, 1, 2, True)
    hidden_one = tokens + matmul(self_att, self_out)
    normed_two = rms_scale(hidden_one, gain_all[1]).astype(jnp.bfloat16)
    cross_query = matmul(normed_two, cross_in).astype(jnp.bfloat16)
    cross_kv = matmul(encoder, cross_kv_in).astype(jnp.bfloat16)
    cross_att, cross_total = attention_forward(cross_query, cross_kv, enc_limit, 0, 0, 1, False)
    hidden_two = hidden_one + matmul(cross_att, cross_out)
    normed_three = rms_scale(hidden_two, gain_all[2]).astype(jnp.bfloat16)
    gate_up = matmul(normed_three, feed_in)
    gate_part, up_part = (gate_up[:, :hidden_units], gate_up[:, hidden_units:])
    activated = gated_unit(gate_part, up_part).astype(jnp.bfloat16)
    result = hidden_two + matmul(activated, feed_out, NT)
    out_tokens = (result * valid_rows).astype(jnp.bfloat16).reshape(1, 1, SEQ_LEN, D)

    cols = (((0,), (0,)), ((), ()))
    grad_result = out_grad[0, 0].astype(jnp.float32) * valid_rows
    grad_branch = grad_result.astype(jnp.bfloat16)
    grad_activated = matmul(grad_branch, feed_out)
    unused, gate_pull = jax.vjp(gated_unit, gate_part, up_part)
    grad_gate, grad_up = gate_pull(grad_activated)
    grad_gate_up = low(grad_gate, grad_up)
    grad_normed = matmul(grad_gate_up, feed_in, NT)
    feed_out_grad = matmul(grad_branch, activated, cols).astype(jnp.bfloat16)
    feed_in_grad = matmul(normed_three, grad_gate_up, cols).astype(jnp.bfloat16)
    grad_normed, feed_out_grad, feed_in_grad = tie((grad_normed, feed_out_grad, feed_in_grad))
    feed_in_part = scatter(feed_in_grad)
    feed_out_part = scatter(feed_out_grad)
    unused, norm_pull = jax.vjp(rms_scale, hidden_two, gain_all[2])
    grad_hidden, grad_gain_three = norm_pull(grad_normed)
    grad_hidden_two = grad_result + grad_hidden

    grad_cross_z = grad_hidden_two.astype(jnp.bfloat16)
    grad_cross_att = matmul(grad_cross_z, cross_out, NT).astype(jnp.bfloat16)
    cross_out_grad = matmul(cross_att, grad_cross_z, cols).astype(jnp.bfloat16)
    grad_cross_att, cross_out_grad = tie((grad_cross_att, cross_out_grad))
    cross_out_sum = links.reduce(cross_out_grad)
    grad_cross_query, grad_cross_kv = attention_backward(
        cross_query, cross_kv, cross_att, grad_cross_att, cross_total, enc_limit, 0, 0, 1, False
    )
    grad_normed_two = matmul(grad_cross_query, cross_in, NT)
    grad_encoder = matmul(grad_cross_kv, cross_kv_in, NT)
    cross_query_grad = matmul(normed_two, grad_cross_query, cols).astype(jnp.bfloat16)
    cross_kv_grad = matmul(encoder, grad_cross_kv, cols).astype(jnp.bfloat16)
    grad_normed_two, grad_encoder, cross_query_grad, cross_kv_grad = tie(
        (grad_normed_two, grad_encoder.astype(jnp.bfloat16), cross_query_grad, cross_kv_grad)
    )
    cross_query_sum = links.reduce(cross_query_grad)
    cross_kv_sum = links.reduce(cross_kv_grad)
    encoder_grad = links.back(grad_encoder, order_row)
    unused, norm_pull = jax.vjp(rms_scale, hidden_one, gain_all[1])
    grad_hidden, grad_gain_two = norm_pull(grad_normed_two)
    grad_hidden_one = grad_hidden_two + grad_hidden

    grad_self_z = grad_hidden_one.astype(jnp.bfloat16)
    grad_self_att = matmul(grad_self_z, self_out, NT).astype(jnp.bfloat16)
    self_out_grad = matmul(self_att, grad_self_z, cols).astype(jnp.bfloat16)
    grad_self_att, self_out_grad = tie((grad_self_att, self_out_grad))
    self_out_sum = links.reduce(self_out_grad)
    (grad_self_qkv,) = attention_backward(
        self_qkv, self_qkv, self_att, grad_self_att, self_total, dec_limit, 0, 1, 2, True
    )
    self_in_grad = matmul(normed_one, grad_self_qkv, cols).astype(jnp.bfloat16)
    grad_self_qkv, self_in_grad = tie((grad_self_qkv, self_in_grad))
    self_in_sum = links.reduce(self_in_grad)
    grad_normed_one = matmul(grad_self_qkv, self_in, NT)
    unused, norm_pull = jax.vjp(rms_scale, tokens, gain_all[0])
    grad_hidden, grad_gain_one = norm_pull(grad_normed_one)
    grad_tokens = grad_hidden_one + grad_hidden
    token_grad = links.back(grad_tokens.astype(jnp.bfloat16), order_row)
    gain_sum = lax.psum(jnp.stack([grad_gain_one, grad_gain_two, grad_gain_three]), ("rep", "fsdp"))
    gain_cols = gain_master.shape[1]
    gain_grad = lax.dynamic_slice_in_dim(gain_sum, links.shard * gain_cols, gain_cols, 1)
    feed_in_sum = links.reduce_rep(feed_in_part)
    feed_out_sum = links.reduce_rep(feed_out_part)
    attn_sum = jnp.concatenate(
        [self_in_sum, self_out_sum, cross_query_sum, cross_kv_sum, cross_out_sum], 1
    )
    attn_grad, attn_update, attn_left_new, attn_right_new = precondition(
        attn_sum, attn_left, attn_right, attn_left_root, attn_right_root, decays[0], 8
    )
    ffin_grad, ffin_update, ffin_left_new, ffin_right_new = precondition(
        feed_in_sum, ffin_left, ffin_right, ffin_left_root, ffin_right_root, decays[1], 2
    )
    ffout_grad, ffout_update, ffout_left_new, ffout_right_new = precondition(
        feed_out_sum, ffout_left, ffout_right, ffout_left_root, ffout_right_root, decays[2], 1
    )
    gain_update, gain_stats_new = update_gains(gain_grad, gain_stats, decays[3])
    return (
        out_tokens,
        token_grad,
        encoder_grad,
        attn_grad,
        ffin_grad,
        ffout_grad,
        gain_grad,
        attn_update,
        ffin_update,
        ffout_update,
        gain_update,
        attn_left_new,
        attn_right_new,
        ffin_left_new,
        ffin_right_new,
        ffout_left_new,
        ffout_right_new,
        gain_stats_new,
    )


def solution(mesh):
    in_specs = (
        P("rep", None, "fsdp", None),
        P("rep", None, "fsdp", None),
        P("rep", "fsdp", None, None),
        P("rep", None),
        P("rep", None),
        P("rep", None),
        P(None, "fsdp", None),
        P(None, "fsdp", None),
        P("fsdp", None),
        P(None, "fsdp"),
        P(),
        P(None, "fsdp", None, None),
        P(None, "fsdp", None, None),
        P(None, "fsdp", None, None),
        P(None, "fsdp", None, None),
        P(None, "fsdp", None, None),
        P(None, "fsdp", None, None),
        P(None, "fsdp", None, None),
        P(None, "fsdp", None, None),
        P("fsdp", None, None),
        P("fsdp", None, None),
        P("fsdp", None, None),
        P("fsdp", None, None),
        P(None, "fsdp"),
    )
    out_specs = (
        P("rep", "fsdp", None, None),
        P("rep", None, "fsdp", None),
        P("rep", None, "fsdp", None),
        P(None, "fsdp", None),
        P(None, "fsdp", None),
        P("fsdp", None),
        P(None, "fsdp"),
        P(None, "fsdp", None),
        P(None, "fsdp", None),
        P("fsdp", None),
        P(None, "fsdp"),
        P(None, "fsdp", None, None),
        P(None, "fsdp", None, None),
        P(None, "fsdp", None, None),
        P(None, "fsdp", None, None),
        P("fsdp", None, None),
        P("fsdp", None, None),
        P(None, "fsdp"),
    )
    return jax.shard_map(functools.partial(body, mesh), mesh=mesh, in_specs=in_specs, out_specs=out_specs, check_vma=False)
```
